32 devices in a mesh: grp: 4 (over x, core), fsdp: 8 (over z, y).
Axes of the slice: x: 2, y: 2, z: 4, core: 2. Of those that a mesh axis runs over, the one named last changes fastest.
Arguments:
- layer_input_rows: bfloat16 [16384, 8192], P(('grp', 'fsdp')), may hold values from -400 to 400, as said below
- input_norm_gain: bfloat16 [8192], replicated, may hold values from 0.5 to 1.5
- key_value_codes: int32 [8192, 256], P('fsdp'), may hold values from 0 to 65535
- block_scale_codes: int32 [256, 128], P('fsdp'), may hold values from -2147483648 to 2147483646
- outer_scale_codes: int32 [512], P('fsdp'), may hold values from 0 to 255
- adapter_down_factor: bfloat16 [8192, 64], replicated, may hold values from -0.0625 to 0.0625
- adapter_up_factor: bfloat16 [64, 1024], replicated, may hold values from -0.75 to 0.75
- target: bfloat16 [16384, 1024], P(('grp', 'fsdp')), may hold values from -18 to 18
Outputs:
- kv: bfloat16 [16384, 1024], P(('grp', 'fsdp'))
- loss: float32 [], replicated
The draws below stay inside these ranges and needn't reach their ends.
Inputs may be any that keep to these rules, and one draw needn't show every extreme that they name: layer_input_rows rows and features carry varied scales.
All inputs are finite; a program needn't handle non-finite values.
Results may differ from the reference program's by a relative error of at most 0.0057.
Values may be sent and summed in bfloat16 or wider, within the bound.
A program may use at most 128 MiB of HBM per device.

```python
import jax
import jax.numpy as jnp
from jax import lax

MODEL_WIDTH = 8192
ADAPTER_RANK = 64
KEY_VALUE_COLS = 1024
GROUP_TOKENS = 4096
TOKENS = 16384
N_GRP = 4


def draw_layer_input_rows(key, part):
    key_noise = jax.random.fold_in(key, 11)
    key_rows = jax.random.fold_in(key, 12)
    key_cols = jax.random.fold_in(key, 13)
    row_scale = jnp.exp(jax.random.uniform(key_rows, (TOKENS, 1), jnp.float32) * jnp.log(10.0))
    col_scale = jnp.exp(jax.random.uniform(key_cols, (1, MODEL_WIDTH), jnp.float32) * jnp.log(10.0))
    noise = jnp.clip(jax.random.normal(key_noise, (TOKENS, MODEL_WIDTH), jnp.float32), -4.0, 4.0)
    return (noise * row_scale * col_scale).astype(jnp.bfloat16)


def draw_target(key, part):
    key_noise = jax.random.fold_in(key, 21)
    position = jnp.arange(TOKENS, dtype=jnp.float32) / TOKENS
    growth = 1.0 + 2.0 * position
    noise = jnp.clip(jax.random.normal(key_noise, (TOKENS, KEY_VALUE_COLS), jnp.float32), -6.0, 6.0)
    return (noise * growth[:, None]).astype(jnp.bfloat16)


def set_ends(result, own_key, low, high):
    longest = result.shape.index(max(result.shape))
    spots = []
    for shift in (0, 1):
        where = [jax.random.randint(jax.random.fold_in(own_key, axis), (), 0, length) for axis, length in enumerate(result.shape)]
        where[longest] = (where[longest] + shift) % result.shape[longest]
        spots.append(tuple(where))
    return result.at[spots[0]].set(low).at[spots[1]].set(high)


def centred(rng, dims, deviation, reach, kind=jnp.bfloat16):
    return jnp.clip(deviation * jax.random.normal(rng, dims, jnp.float32), -reach, reach).astype(kind)


def setup_inputs(seed: int = 0) -> dict:
    seeds = jax.random.split(jax.random.key(seed), 9)
    return {
        "layer_input_rows": draw_layer_input_rows(jax.random.fold_in(seeds[8], 71), 0),
        "input_norm_gain": jnp.clip(1.0 + 0.1 * jax.random.normal(seeds[1], (MODEL_WIDTH,), jnp.float32), 0.5, 1.5).astype(jnp.bfloat16),
        "key_value_codes": set_ends(jax.random.randint(seeds[2], (MODEL_WIDTH, KEY_VALUE_COLS // 4), 0, 65536), jax.random.fold_in(seeds[2], 1), 0, 65535).astype(jnp.int32),
        "block_scale_codes": set_ends(jax.random.randint(seeds[3], (MODEL_WIDTH * KEY_VALUE_COLS // 32768, 128), -2147483648, 2147483647), jax.random.fold_in(seeds[3], 1), -2147483648, 2147483646).astype(jnp.int32),
        "outer_scale_codes": set_ends(jax.random.randint(seeds[4], (MODEL_WIDTH * KEY_VALUE_COLS // 16384,), 0, 256), jax.random.fold_in(seeds[4], 1), 0, 255).astype(jnp.int32),
        "adapter_down_factor": centred(seeds[5], (MODEL_WIDTH, ADAPTER_RANK), MODEL_WIDTH ** -0.5, 0.0625),
        "adapter_up_factor": centred(seeds[6], (ADAPTER_RANK, KEY_VALUE_COLS), ADAPTER_RANK ** -0.5, 0.75),
        "target": draw_target(jax.random.fold_in(seeds[8], 71), 0),
    }


adapter_scale = 0.25
epsilon = 1e-06
nf4_levels = (-1.0, -0.6961928009986877, -0.5250730514526367, -0.39491748809814453, -0.28444138169288635, -0.18477343022823334, -0.09105003625154495, 0.0, 0.07958029955625534, 0.16093020141124725, 0.24611230194568634, 0.33791524171066284, 0.44070982933044434, 0.5626170039176941, 0.7229568362236023, 1.0)

def unpack_scales(code_words, outer_scale_codes, all_rows):
    per_row = code_words.size // all_rows
    flat = code_words.reshape(all_rows, per_row)
    shifts = jnp.arange(4, dtype=jnp.int32) * 8
    code_bytes = jnp.bitwise_and(jnp.right_shift(flat[:, :, None], shifts[None, None, :]), 255)
    code_bytes = code_bytes.reshape(all_rows, per_row * 4).astype(jnp.float32)
    group_rows = all_rows // outer_scale_codes.shape[0]
    second = jnp.exp2(outer_scale_codes.astype(jnp.float32) / 128.0 - 6.0)
    second = jnp.repeat(second, group_rows)
    return (code_bytes + 0.5) / 256.0 * second[:, None]

def decode_codes(words, absmax):
    height = words.shape[0]
    shifts = jnp.arange(4, dtype=jnp.int32) * 4
    nibbles = jnp.bitwise_and(jnp.right_shift(words[:, :, None], shifts[None, None, :]), 15)
    nibbles = nibbles.reshape(height, words.shape[1] * 4)
    values = jnp.zeros(nibbles.shape, jnp.float32)
    for number, level in enumerate(nf4_levels):
        values = jnp.where(nibbles == number, jnp.float32(level), values)
    width = values.shape[1]
    count = absmax.shape[1]
    scaled = values.reshape(height, count, width // count) * absmax[:, :, None]
    return scaled.reshape(height, width).astype(jnp.bfloat16)

def apply_input_norm(input_states, input_norm_gain):
    values = input_states.astype(jnp.float32)
    inverse = lax.rsqrt(lax.optimization_barrier(jnp.mean(values * values, axis=1, keepdims=True)) + epsilon)
    return (values * inverse * input_norm_gain.astype(jnp.float32)[None, :]).astype(jnp.bfloat16)

def key_value_project(normed_input, decoded_weight, adapter_down_factor, adapter_up_factor):
    frozen_output = jnp.dot(normed_input, decoded_weight, preferred_element_type=jnp.float32)
    adapter_output = jnp.dot(normed_input, adapter_down_factor, preferred_element_type=jnp.float32).astype(jnp.bfloat16)
    return frozen_output + adapter_scale * jnp.dot(adapter_output, adapter_up_factor, preferred_element_type=jnp.float32)

def reference(layer_input_rows, input_norm_gain, key_value_codes, block_scale_codes, outer_scale_codes, adapter_down_factor, adapter_up_factor, target):
    absmax = unpack_scales(block_scale_codes, outer_scale_codes, key_value_codes.shape[0])
    decoded_weight = decode_codes(key_value_codes, absmax)

    def one_group(pair):
        input_states, teacher = pair
        precise_output = key_value_project(apply_input_norm(input_states, input_norm_gain), decoded_weight, adapter_down_factor, adapter_up_factor)
        error_terms = precise_output - teacher.astype(jnp.float32)
        return (precise_output.astype(jnp.bfloat16), jnp.sum(error_terms * error_terms) / (GROUP_TOKENS * KEY_VALUE_COLS))
    kv_out, losses = lax.map(one_group, (layer_input_rows.reshape(N_GRP, GROUP_TOKENS, MODEL_WIDTH), target.reshape(N_GRP, GROUP_TOKENS, KEY_VALUE_COLS)))
    return (kv_out.reshape(TOKENS, KEY_VALUE_COLS), jnp.sum(losses))
```

```python
import functools

import jax
import jax.numpy as jnp
from jax import lax
from jax.experimental import pallas as pl
from jax.experimental.pallas import tpu as pltpu
from jax.sharding import PartitionSpec as P

adapter_scale = 0.25
epsilon = 1e-06
nf4_levels = (
    -1.0,
    -0.6961928009986877,
    -0.5250730514526367,
    -0.39491748809814453,
    -0.28444138169288635,
    -0.18477343022823334,
    -0.09105003625154495,
    0.0,
    0.07958029955625534,
    0.16093020141124725,
    0.24611230194568634,
    0.33791524171066284,
    0.44070982933044434,
    0.5626170039176941,
    0.7229568362236023,
    1.0,
)
MESH = pl.DeviceIdType.MESH


def nibble_levels(words, plane):
    values = [jnp.float32(level) for level in nf4_levels]
    for bit in range(4):
        is_set = jnp.bitwise_and(words, 1 << (4 * plane + bit)) != 0
        values = [
            jnp.where(is_set, values[2 * i + 1], values[2 * i])
            for i in range(len(values) // 2)
        ]
    return values[0]


def kernel(
    layers,
    x_hbm,
    gain_ref,
    codes_ref,
    scales_ref,
    outer_ref,
    down_hbm,
    up_ref,
    target_hbm,
    out_ref,
    loss_ref,
    x_ref,
    weight_ref,
    acc_ref,
    target_ref,
    down_ref,
    spread_ref,
    scale_ref,
    local_sem,
    z_send,
    x_send,
    y_send,
    own_send,
    core_send,
    link_recv,
    core_recv,
):
    g = lax.axis_index("grp")
    f = lax.axis_index("fsdp")
    cx, cc = g // 2, g % 2
    cl, cy = f // 2, f % 2
    tokens, width = x_ref.shape
    columns = acc_ref.shape[1]
    rows = codes_ref.shape[0]
    half = rows // 2
    piece = half // 4

    sibling = (cx * 2 + 1 - cc, f)
    x_peer = ((1 - cx) * 2 + cc, f)
    y_peer = (g, cl * 2 + 1 - cy)

    def z_peer(step):
        return (g, (cl + step) * 2 + cy)

    part = tokens // 4
    x_copies = [
        pltpu.make_async_copy(
            x_hbm.at[pl.ds(p * part, part)], x_ref.at[pl.ds(p * part, part)], local_sem.at[p]
        )
        for p in range(4)
    ]
    target_copy = pltpu.make_async_copy(target_hbm, target_ref, local_sem.at[4])
    down_copy = pltpu.make_async_copy(down_hbm, down_ref, local_sem.at[5])
    for copy in x_copies:
        copy.start()
    down_copy.start()
    target_copy.start()

    barrier = pltpu.get_barrier_semaphore()
    for peer in (sibling, x_peer, y_peer):
        pl.semaphore_signal(barrier, inc=1, device_id=peer, device_id_type=MESH)

    @pl.when(cl > 0)
    def _():
        pl.semaphore_signal(barrier, inc=1, device_id=z_peer(-1), device_id_type=MESH)

    @pl.when(cl < layers - 1)
    def _():
        pl.semaphore_signal(barrier, inc=1, device_id=z_peer(1), device_id_type=MESH)

    def mirror(px, j):
        return j + px * (3 - 2 * j)

    def chunk(layer, y, c, q):
        start = ((layer * 2 + y) * 2 + c) * half + q * piece
        return weight_ref.at[pl.ds(pl.multiple_of(start, piece), piece)]

    def slot(layer, y, q):
        return (layer * 2 + y) * 4 + q

    def link_copy(layer, y, q, send_sem, peer):
        ref = chunk(layer, y, cc, q)
        return pltpu.make_async_remote_copy(
            src_ref=ref,
            dst_ref=ref,
            send_sem=send_sem,
            recv_sem=link_recv.at[slot(layer, y, q)],
            device_id=peer,
            device_id_type=MESH,
        )

    def z_copy(layer, j, step):
        sem = z_send.at[(1 + step) // 2 * (layers * 3) + layer * 3 + j]
        return link_copy(layer, cy, mirror(cx, j), sem, z_peer(step))

    def xz_copy(layer):
        return link_copy(layer, cy, mirror(cx, 0), x_send.at[layer * 3], x_peer)

    def xy_copy(layer, j):
        return link_copy(layer, 1 - cy, mirror(cx, j), x_send.at[layer * 3 + 1 + j], x_peer)

    def y_copy(layer, j):
        return link_copy(layer, cy, mirror(cx, j), y_send.at[layer * 2 + j], y_peer)

    def own_copy(k):
        return link_copy(cl, cy, k, own_send.at[k], y_peer)

    def core_copy(layer, y, q):
        ref = chunk(layer, y, cc, q)
        place = slot(layer, y, q)
        return pltpu.make_async_remote_copy(
            src_ref=ref,
            dst_ref=ref,
            send_sem=core_send.at[place],
            recv_sem=core_recv.at[place],
            device_id=sibling,
            device_id_type=MESH,
        )

    def arrived(layer, y, q):
        ref = chunk(layer, y, cc, q)
        pltpu.make_async_copy(ref, ref, link_recv.at[slot(layer, y, q)]).wait()

    def core_arrived(layer, y, q):
        ref = chunk(layer, y, 1 - cc, q)
        pltpu.make_async_copy(ref, ref, core_recv.at[slot(layer, y, q)]).wait()

    words = codes_ref.shape[1]
    lanes = scales_ref.shape[1]
    per_row = scales_ref.shape[0] * lanes // rows
    line = rows // scales_ref.shape[0]
    row = lax.broadcasted_iota(jnp.int32, (rows, lanes), 0)
    lane = lax.broadcasted_iota(jnp.int32, (rows, lanes), 1)
    mine = lane // per_row == row % line
    place = lax.broadcasted_iota(jnp.int32, (lanes, words), 0)
    word = lax.broadcasted_iota(jnp.int32, (lanes, words), 1)
    run = words // (4 * per_row)
    code = jnp.zeros((rows, words), jnp.float32)
    scale_words = jnp.concatenate(
        [
            jnp.broadcast_to(scales_ref[pl.ds(i, 1), :], (line, lanes))
            for i in range(scales_ref.shape[0])
        ],
        axis=0,
    )
    for byte in range(4):
        value = jnp.bitwise_and(jnp.right_shift(scale_words, 8 * byte), 255)
        value = jnp.where(mine, value.astype(jnp.float32), 0.0).astype(jnp.bfloat16)
        pick = (place % per_row == word // (4 * run)) & ((word // run) % 4 == byte)
        code += jnp.dot(
            value,
            jnp.where(pick, 1.0, 0.0).astype(jnp.bfloat16),
            preferred_element_type=jnp.float32,
        )
    outer_count = outer_ref.shape[1]
    outer_rows = rows // outer_count
    outer_row = lax.broadcasted_iota(jnp.int32, (rows, outer_count), 0)
    outer_lane = lax.broadcasted_iota(jnp.int32, (rows, outer_count), 1)
    second = jnp.sum(
        jnp.where(
            outer_row // outer_rows == outer_lane, outer_ref[...].astype(jnp.float32), 0.0
        ),
        axis=1,
        keepdims=True,
    )
    second = jnp.exp2(second / 128.0 - 6.0)
    scale_ref[...] = (code + 0.5) / 256.0 * second

    deep = lax.broadcasted_iota(jnp.int32, spread_ref.shape, 0)
    wide = lax.broadcasted_iota(jnp.int32, spread_ref.shape, 1)
    spread_ref[...] = jnp.where(
        (deep % 128) * 4 + deep // 128 == wide, 1.0, 0.0
    ).astype(jnp.bfloat16)

    def decode(start):
        start = pl.multiple_of(start, piece)
        for h in range(words // 128):
            span = pl.ds(h * 128, 128)
            code_words = codes_ref[pl.ds(start, piece), span]
            scale = scale_ref[pl.ds(start, piece), span]
            planes = [
                (nibble_levels(code_words, plane) * scale).astype(jnp.bfloat16)
                for plane in range(4)
            ]
            ordered = jnp.dot(
                jnp.concatenate(planes, axis=1),
                spread_ref[...],
                preferred_element_type=jnp.float32,
            )
            weight_ref[
                pl.ds(pl.multiple_of(f * rows + start, piece), piece), pl.ds(h * 512, 512)
            ] = ordered.astype(jnp.bfloat16)

    decode(cc * half + mirror(cx, 0) * piece)
    pl.semaphore_wait(
        barrier, 3 + (cl > 0).astype(jnp.int32) + (cl < layers - 1).astype(jnp.int32)
    )

    def first_sends(j):
        @pl.when(cl > 0)
        def _():
            z_copy(cl, j, -1).start()

        @pl.when(cl < layers - 1)
        def _():
            z_copy(cl, j, 1).start()

    def rest(j, carry):
        decode(cc * half + mirror(cx, j) * piece)
        first_sends(j - 1)
        return carry

    lax.fori_loop(1, 4, rest, 0)
    own_copy(0).start()
    for k in range(layers, 4):
        own_copy(k).start()

    def other(j, carry):
        decode((1 - cc) * half + j * piece)
        return carry

    lax.fori_loop(0, 4, other, 0)

    block = min(16, part)
    tile = min(1024, width)

    def normalize(p):
        x_copies[p].wait()

        def some(i, carry):
            at = pl.ds(pl.multiple_of(p * part + i * block, block), block)
            total = jnp.zeros((block, 128), jnp.float32)
            for t in range(width // tile):
                v = x_ref[at, pl.ds(t * tile, tile)].astype(jnp.float32)
                v = v * v
                for k in range(tile // 128):
                    total += v[:, k * 128 : (k + 1) * 128]
            inverse = lax.rsqrt(jnp.sum(total, axis=1, keepdims=True) / width + epsilon)
            for t in range(width // tile):
                span = pl.ds(t * tile, tile)
                v = x_ref[at, span].astype(jnp.float32)
                x_ref[at, span] = (v * inverse * gain_ref[:, span].astype(jnp.float32)).astype(
                    jnp.bfloat16
                )
            return carry

        lax.fori_loop(0, part // block, some, 0)

    def adapter():
        down_copy.wait()
        low = jnp.dot(x_ref[...], down_ref[...], preferred_element_type=jnp.float32)
        acc_ref[...] = adapter_scale * jnp.dot(
            low.astype(jnp.bfloat16), up_ref[...], preferred_element_type=jnp.float32
        )

    across = min(256, columns)

    def multiply(layer, y):
        at = pl.ds(pl.multiple_of((layer * 2 + y) * rows, rows), rows)

        def some(n, carry):
            cols = pl.ds(pl.multiple_of(n * across, across), across)
            acc_ref[:, cols] += jnp.dot(
                x_ref[:, at], weight_ref[at, cols], preferred_element_type=jnp.float32
            )
            return carry

        lax.fori_loop(0, columns // across, some, 0)

    def multiply_arrived(layer, y):
        for q in range(4):
            core_arrived(layer, y, q)
        multiply(layer, y)

    def both(s, act):
        for step in (-1, 1):
            layer = cl + step * s
            pl.when((layer >= 0) & (layer < layers))(functools.partial(act, layer, step))

    def z_event(s, j):
        def act(layer, step):
            arrived(layer, cy, mirror(cx, j))
            onward = cl - step

            @pl.when((onward >= 0) & (onward < layers))
            def _():
                z_copy(layer, j, -step).start()

            if j == 0:
                xz_copy(layer).start()
            if j < 2:
                y_copy(layer, j).start()
            core_copy(layer, cy, mirror(cx, j)).start()

        both(s, act)

    def y_event(s, j):
        def act(layer, step):
            q = mirror(cx, j)
            arrived(layer, 1 - cy, q)
            xy_copy(layer, j).start()
            core_copy(layer, 1 - cy, q).start()

        both(s, act)

    def xz_event(s):
        def act(layer, step):
            q = mirror(1 - cx, 0)
            arrived(layer, cy, q)
            core_copy(layer, cy, q).start()

        both(s, act)

    def xy_event(s, j):
        def act(layer, step):
            q = mirror(1 - cx, j)
            arrived(layer, 1 - cy, q)
            core_copy(layer, 1 - cy, q).start()

        both(s, act)

    def own_event(k):
        arrived(cl, 1 - cy, k)
        core_copy(cl, 1 - cy, k).start()

    def one_step(s, carry):
        z_event(s, 0)
        pl.when(s <= 4)(lambda: own_event(s - 1))

        @pl.when(s > 1)
        def _():
            xy_event(s - 1, 1)
            both(s - 1, lambda layer, step: multiply_arrived(layer, cy))

        @pl.when(s == 1)
        def _():
            normalize(0)
            normalize(1)

        z_event(s, 1)
        y_event(s, 0)
        xz_event(s)

        @pl.when(s > 1)
        def _():
            both(s - 1, lambda layer, step: multiply_arrived(layer, 1 - cy))

        @pl.when(s == 1)
        def _():
            normalize(2)
            normalize(3)

        z_event(s, 2)
        pl.when(s < 4)(lambda: own_copy(s).start())
        y_event(s, 1)
        xy_event(s, 0)

        @pl.when(s == 1)
        def _():
            adapter()
            multiply(cl, cy)

        return carry

    lax.fori_loop(1, layers, one_step, 0)
    for k in range(min(layers - 1, 4), 4):
        own_event(k)
    xy_event(layers - 1, 1)
    both(layers - 1, lambda layer, step: multiply_arrived(layer, cy))
    multiply_arrived(cl, 1 - cy)
    both(layers - 1, lambda layer, step: multiply_arrived(layer, 1 - cy))

    target_copy.wait()
    loss_ref[...] = jnp.zeros_like(loss_ref)

    def finish(i, carry):
        at = pl.ds(pl.multiple_of(i * block, block), block)
        exact = acc_ref[at, :]
        out_ref[at, :] = exact.astype(jnp.bfloat16)
        error = exact - target_ref[at, :].astype(jnp.float32)
        error = error * error
        total = jnp.zeros((block, 128), jnp.float32)
        for k in range(columns // 128):
            total += error[:, k * 128 : (k + 1) * 128]
        for k in range(block // 8):
            loss_ref[...] += total[k * 8 : (k + 1) * 8]
        return carry

    lax.fori_loop(0, tokens // block, finish, 0)

    for j in range(3):
        for step in (-1, 1):

            @pl.when((cl + step >= 0) & (cl + step < layers))
            def _():
                z_copy(cl, j, step).wait_send()

    def sent(s, carry):
        def act(layer, step):
            onward = cl - step

            @pl.when((onward >= 0) & (onward < layers))
            def _():
                for j in range(3):
                    z_copy(layer, j, -step).wait_send()

            xz_copy(layer).wait_send()
            for j in range(2):
                y_copy(layer, j).wait_send()
                xy_copy(layer, j).wait_send()
            for q in range(4):
                core_copy(layer, cy, q).wait_send()
                core_copy(layer, 1 - cy, q).wait_send()

        both(s, act)
        return carry

    lax.fori_loop(1, layers, sent, 0)
    for k in range(4):
        own_copy(k).wait_send()
        core_copy(cl, 1 - cy, k).wait_send()


def per_device(fsdp, x, gain, codes, scales, outer, down, up, target):
    tokens, width = x.shape
    columns = up.shape[1]
    rows = codes.shape[0]
    layers = fsdp // 2
    vmem = pl.BlockSpec(memory_space=pltpu.VMEM)
    anywhere = pl.BlockSpec(memory_space=pl.ANY)
    dma = pltpu.SemaphoreType.DMA
    kv, squares = pl.pallas_call(
        functools.partial(kernel, layers),
        out_shape=(
            jax.ShapeDtypeStruct((tokens, columns), jnp.bfloat16),
            jax.ShapeDtypeStruct((8, 128), jnp.float32),
        ),
        in_specs=[anywhere, vmem, vmem, vmem, vmem, anywhere, vmem, anywhere],
        out_specs=(vmem, vmem),
        scratch_shapes=[
            pltpu.VMEM((tokens, width), jnp.bfloat16),
            pltpu.VMEM((width, columns), jnp.bfloat16),
            pltpu.VMEM((tokens, columns), jnp.float32),
            pltpu.VMEM((tokens, columns), jnp.bfloat16),
            pltpu.VMEM(down.shape, jnp.bfloat16),
            pltpu.VMEM((512, 512), jnp.bfloat16),
            pltpu.VMEM(codes.shape, jnp.float32),
            dma((6,)),
            dma((2 * layers * 3,)),
            dma((layers * 3,)),
            dma((layers * 2,)),
            dma((4,)),
            dma((layers * 8,)),
            dma((layers * 8,)),
            dma((layers * 8,)),
        ],
        compiler_params=pltpu.CompilerParams(
            collective_id=0, has_side_effects=True, vmem_limit_bytes=60 * 1024 * 1024
        ),
    )(x, gain.reshape(1, width), codes, scales, outer.reshape(1, -1), down, up, target)
    partial_value = jnp.sum(squares) / (tokens * fsdp * columns)
    return kv, lax.psum(partial_value, ("grp", "fsdp"))


def solution(mesh):
    placed = (
        P(("grp", "fsdp"), None),
        P(),
        P("fsdp", None),
        P("fsdp", None),
        P("fsdp"),
        P(),
        P(),
        P(("grp", "fsdp"), None),
    )
    return jax.shard_map(
        functools.partial(per_device, mesh.shape["fsdp"]),
        mesh=mesh,
        in_specs=placed,
        out_specs=(P(("grp", "fsdp"), None), P()),
        check_vma=False,
    )
```

```python
import functools

import jax
import jax.numpy as jnp
from jax import lax
from jax.experimental import pallas as pl
from jax.experimental.pallas import tpu as pltpu
from jax.sharding import PartitionSpec as P

adapter_scale = 0.25
epsilon = 1e-06
nf4_levels = (
    -1.0,
    -0.6961928009986877,
    -0.5250730514526367,
    -0.39491748809814453,
    -0.28444138169288635,
    -0.18477343022823334,
    -0.09105003625154495,
    0.0,
    0.07958029955625534,
    0.16093020141124725,
    0.24611230194568634,
    0.33791524171066284,
    0.44070982933044434,
    0.5626170039176941,
    0.7229568362236023,
    1.0,
)
MESH = pl.DeviceIdType.MESH


def nibble_levels(words, plane):
    values = [jnp.float32(level) for level in nf4_levels]
    for bit in range(4):
        is_set = jnp.bitwise_and(words, 1 << (4 * plane + bit)) != 0
        values = [
            jnp.where(is_set, values[2 * i + 1], values[2 * i])
            for i in range(len(values) // 2)
        ]
    return values[0]


def kernel(
    layers,
    x_hbm,
    gain_ref,
    codes_ref,
    scales_ref,
    outer_ref,
    down_hbm,
    up_ref,
    target_hbm,
    out_ref,
    loss_ref,
    x_ref,
    weight_ref,
    acc_ref,
    target_ref,
    down_ref,
    spread_ref,
    scale_ref,
    wide_gain_ref,
    plane_ref,
    line_ref,
    local_sem,
    z_send,
    x_send,
    y_send,
    own_send,
    core_send,
    link_recv,
    core_recv,
    plane_send,
    plane_recv,
    line_send,
    line_recv,
):
    g = lax.axis_index("grp")
    f = lax.axis_index("fsdp")
    cx, cc = g // 2, g % 2
    cl, cy = f // 2, f % 2
    tokens, width = x_ref.shape
    columns = acc_ref.shape[1]
    rows = codes_ref.shape[0]
    half = rows // 2
    piece = half // 4

    sibling = (cx * 2 + 1 - cc, f)
    x_peer = ((1 - cx) * 2 + cc, f)
    y_peer = (g, cl * 2 + 1 - cy)

    def z_peer(step):
        return (g, (cl + step) * 2 + cy)

    part = tokens // 4
    x_copies = [
        pltpu.make_async_copy(
            x_hbm.at[pl.ds(p * part, part)], x_ref.at[pl.ds(p * part, part)], local_sem.at[p]
        )
        for p in range(4)
    ]
    target_copy = pltpu.make_async_copy(target_hbm, target_ref, local_sem.at[4])
    down_copy = pltpu.make_async_copy(down_hbm, down_ref, local_sem.at[5])
    for copy in x_copies:
        copy.start()
    down_copy.start()
    target_copy.start()

    barrier = pltpu.get_barrier_semaphore()
    spot = (cx * 2 + cc) * 2 + cy

    def plane_peer(i):
        to = (spot + i) % 8
        return (to // 2, cl * 2 + to % 2)

    def line_peer(i):
        return (g, (cl + i) % layers * 2 + cy)

    for i in range(1, 8):
        pl.semaphore_signal(barrier, inc=1, device_id=plane_peer(i), device_id_type=MESH)

    def greet(i, carry):
        pl.semaphore_signal(barrier, inc=1, device_id=line_peer(i), device_id_type=MESH)
        return carry

    lax.fori_loop(1, layers, greet, 0)

    def mirror(px, j):
        return j + px * (3 - 2 * j)

    def chunk(layer, y, c, q):
        start = ((layer * 2 + y) * 2 + c) * half + q * piece
        return weight_ref.at[pl.ds(pl.multiple_of(start, piece), piece)]

    def slot(layer, y, q):
        return (layer * 2 + y) * 4 + q

    def link_copy(layer, y, q, send_sem, peer):
        ref = chunk(layer, y, cc, q)
        return pltpu.make_async_remote_copy(
            src_ref=ref,
            dst_ref=ref,
            send_sem=send_sem,
            recv_sem=link_recv.at[slot(layer, y, q)],
            device_id=peer,
            device_id_type=MESH,
        )

    def z_copy(layer, j, step):
        sem = z_send.at[(1 + step) // 2 * (layers * 3) + layer * 3 + j]
        return link_copy(layer, cy, mirror(cx, j), sem, z_peer(step))

    def xz_copy(layer):
        return link_copy(layer, cy, mirror(cx, 0), x_send.at[layer * 3], x_peer)

    def xy_copy(layer, j):
        return link_copy(layer, 1 - cy, mirror(cx, j), x_send.at[layer * 3 + 1 + j], x_peer)

    def y_copy(layer, j):
        return link_copy(layer, cy, mirror(cx, j), y_send.at[layer * 2 + j], y_peer)

    def own_copy(k):
        return link_copy(cl, cy, mirror(cx, k), own_send.at[k], y_peer)

    def core_copy(layer, y, q):
        ref = chunk(layer, y, cc, q)
        place = slot(layer, y, q)
        return pltpu.make_async_remote_copy(
            src_ref=ref,
            dst_ref=ref,
            send_sem=core_send.at[place],
            recv_sem=core_recv.at[place],
            device_id=sibling,
            device_id_type=MESH,
        )

    def arrived(layer, y, q):
        ref = chunk(layer, y, cc, q)
        pltpu.make_async_copy(ref, ref, link_recv.at[slot(layer, y, q)]).wait()

    def core_arrived(layer, y, q):
        ref = chunk(layer, y, 1 - cc, q)
        pltpu.make_async_copy(ref, ref, core_recv.at[slot(layer, y, q)]).wait()

    wide_gain_ref[...] = gain_ref[...].astype(jnp.float32)

    words = codes_ref.shape[1]
    lanes = scales_ref.shape[1]
    per_row = scales_ref.shape[0] * lanes // rows
    line = rows // scales_ref.shape[0]
    row = lax.broadcasted_iota(jnp.int32, (rows, lanes), 0)
    lane = lax.broadcasted_iota(jnp.int32, (rows, lanes), 1)
    mine = lane // per_row == row % line
    place = lax.broadcasted_iota(jnp.int32, (lanes, words), 0)
    word = lax.broadcasted_iota(jnp.int32, (lanes, words), 1)
    run = words // (4 * per_row)
    code = jnp.zeros((rows, words), jnp.float32)
    scale_words = jnp.concatenate(
        [
            jnp.broadcast_to(scales_ref[pl.ds(i, 1), :], (line, lanes))
            for i in range(scales_ref.shape[0])
        ],
        axis=0,
    )
    for byte in range(4):
        value = jnp.bitwise_and(jnp.right_shift(scale_words, 8 * byte), 255)
        value = jnp.where(mine, value.astype(jnp.float32), 0.0).astype(jnp.bfloat16)
        pick = (place % per_row == word // (4 * run)) & ((word // run) % 4 == byte)
        code += jnp.dot(
            value,
            jnp.where(pick, 1.0, 0.0).astype(jnp.bfloat16),
            preferred_element_type=jnp.float32,
        )
    outer_count = outer_ref.shape[1]
    outer_rows = rows // outer_count
    outer_row = lax.broadcasted_iota(jnp.int32, (rows, outer_count), 0)
    outer_lane = lax.broadcasted_iota(jnp.int32, (rows, outer_count), 1)
    second = jnp.sum(
        jnp.where(
            outer_row // outer_rows == outer_lane, outer_ref[...].astype(jnp.float32), 0.0
        ),
        axis=1,
        keepdims=True,
    )
    second = jnp.exp2(second / 128.0 - 6.0)
    scale_ref[...] = (code + 0.5) / 256.0 * second

    deep = lax.broadcasted_iota(jnp.int32, spread_ref.shape, 0)
    wide = lax.broadcasted_iota(jnp.int32, spread_ref.shape, 1)
    spread_ref[...] = jnp.where(
        (deep % 128) * 4 + deep // 128 == wide, 1.0, 0.0
    ).astype(jnp.bfloat16)

    def decode(start):
        start = pl.multiple_of(start, piece)
        for h in range(words // 128):
            span = pl.ds(h * 128, 128)
            code_words = codes_ref[pl.ds(start, piece), span]
            scale = scale_ref[pl.ds(start, piece), span]
            planes = [
                (nibble_levels(code_words, plane) * scale).astype(jnp.bfloat16)
                for plane in range(4)
            ]
            ordered = jnp.dot(
                jnp.concatenate(planes, axis=1),
                spread_ref[...],
                preferred_element_type=jnp.float32,
            )
            weight_ref[
                pl.ds(pl.multiple_of(f * rows + start, piece), piece), pl.ds(h * 512, 512)
            ] = ordered.astype(jnp.bfloat16)

    decode(cc * half + mirror(cx, 0) * piece)
    pl.semaphore_wait(barrier, 7 + layers - 1)

    def first_sends(j):
        @pl.when(cl > 0)
        def _():
            z_copy(cl, j, -1).start()

        @pl.when(cl < layers - 1)
        def _():
            z_copy(cl, j, 1).start()

        pl.when(j == 0)(lambda: own_copy(0).start())

    def rest(j, carry):
        decode(cc * half + mirror(cx, j) * piece)
        first_sends(j - 1)
        return carry

    lax.fori_loop(1, 4, rest, 0)
    for k in range(layers, 4):
        own_copy(k).start()

    def other(j, carry):
        decode((1 - cc) * half + j * piece)
        return carry

    lax.fori_loop(0, 4, other, 0)

    block = min(16, part)
    tile = min(1024, width)

    def normalize(p):
        x_copies[p].wait()

        def some(i, carry):
            at = pl.ds(pl.multiple_of(p * part + i * block, block), block)
            total = jnp.zeros((block, 128), jnp.float32)
            for t in range(width // tile):
                v = x_ref[at, pl.ds(t * tile, tile)].astype(jnp.float32)
                v = v * v
                for k in range(tile // 128):
                    total += v[:, k * 128 : (k + 1) * 128]
            inverse = lax.rsqrt(jnp.sum(total, axis=1, keepdims=True) / width + epsilon)
            for t in range(width // 128):
                span = pl.ds(t * 128, 128)
                v = x_ref[at, span].astype(jnp.float32)
                x_ref[at, span] = (v * inverse * wide_gain_ref[pl.ds(t, 1), :]).astype(jnp.bfloat16)
            return carry

        lax.fori_loop(0, part // block, some, 0)

    def adapter():
        down_copy.wait()
        low = lax.dot_general(
            x_ref[...],
            down_ref[...],
            (((1,), (1,)), ((), ())),
            preferred_element_type=jnp.float32,
        )
        acc_ref[...] = adapter_scale * jnp.dot(
            low.astype(jnp.bfloat16), up_ref[...], preferred_element_type=jnp.float32
        )

    across = min(256, columns)

    def multiply(layer, y):
        at = pl.ds(pl.multiple_of((layer * 2 + y) * rows, rows), rows)

        def some(n, carry):
            cols = pl.ds(pl.multiple_of(n * across, across), across)
            acc_ref[:, cols] += jnp.dot(
                x_ref[:, at], weight_ref[at, cols], preferred_element_type=jnp.float32
            )
            return carry

        lax.fori_loop(0, columns // across, some, 0)

    def multiply_arrived(layer, y):
        for q in range(4):
            core_arrived(layer, y, q)
        multiply(layer, y)

    def both(s, act):
        for step in (-1, 1):
            layer = cl + step * s
            pl.when((layer >= 0) & (layer < layers))(functools.partial(act, layer, step))

    def z_event(s, j):
        def act(layer, step):
            arrived(layer, cy, mirror(cx, j))
            onward = cl - step

            @pl.when((onward >= 0) & (onward < layers))
            def _():
                z_copy(layer, j, -step).start()

            if j == 0:
                xz_copy(layer).start()
            if j < 2:
                y_copy(layer, j).start()
            core_copy(layer, cy, mirror(cx, j)).start()

        both(s, act)

    def y_event(s, j):
        def act(layer, step):
            q = mirror(cx, j)
            arrived(layer, 1 - cy, q)
            xy_copy(layer, j).start()
            core_copy(layer, 1 - cy, q).start()

        both(s, act)

    def xz_event(s):
        def act(layer, step):
            q = mirror(1 - cx, 0)
            arrived(layer, cy, q)
            core_copy(layer, cy, q).start()

        both(s, act)

    def xy_event(s, j):
        def act(layer, step):
            q = mirror(1 - cx, j)
            arrived(layer, 1 - cy, q)
            core_copy(layer, 1 - cy, q).start()

        both(s, act)

    def own_event(k):
        q = mirror(cx, k)
        arrived(cl, 1 - cy, q)
        core_copy(cl, 1 - cy, q).start()

    def one_step(s, carry):
        z_event(s, 0)
        pl.when(s <= 4)(lambda: own_event(s - 1))

        @pl.when(s > 1)
        def _():
            xy_event(s - 1, 1)
            both(s - 1, lambda layer, step: multiply_arrived(layer, cy))

        @pl.when(s == 1)
        def _():
            normalize(0)
            normalize(1)

        z_event(s, 1)
        y_event(s, 0)
        xz_event(s)

        @pl.when(s > 1)
        def _():
            both(s - 1, lambda layer, step: multiply_arrived(layer, 1 - cy))

        @pl.when(s == 1)
        def _():
            normalize(2)
            normalize(3)

        z_event(s, 2)
        pl.when(s < 4)(lambda: own_copy(s).start())
        y_event(s, 1)
        xy_event(s, 0)

        @pl.when(s == 1)
        def _():
            adapter()
            multiply(cl, cy)

        return carry

    lax.fori_loop(1, layers, one_step, 0)
    both(layers - 1, lambda layer, step: multiply_arrived(layer, cy))
    for k in range(min(layers - 1, 4), 4):
        own_event(k)
    xy_event(layers - 1, 1)
    multiply_arrived(cl, 1 - cy)
    both(layers - 1, lambda layer, step: multiply_arrived(layer, 1 - cy))

    target_copy.wait()
    plane_ref[spot] = jnp.zeros((8, 128), jnp.float32)

    def finish(i, carry):
        at = pl.ds(pl.multiple_of(i * block, block), block)
        exact = acc_ref[at, :]
        out_ref[at, :] = exact.astype(jnp.bfloat16)
        error = exact - target_ref[at, :].astype(jnp.float32)
        error = error * error
        total = jnp.zeros((block, 128), jnp.float32)
        for k in range(columns // 128):
            total += error[:, k * 128 : (k + 1) * 128]
        for k in range(block // 8):
            plane_ref[spot] += total[k * 8 : (k + 1) * 8]
        return carry

    lax.fori_loop(0, tokens // block, finish, 0)

    for j in range(3):
        for step in (-1, 1):

            @pl.when((cl + step >= 0) & (cl + step < layers))
            def _():
                z_copy(cl, j, step).wait_send()

    def sent(s, carry):
        def act(layer, step):
            onward = cl - step

            @pl.when((onward >= 0) & (onward < layers))
            def _():
                for j in range(3):
                    z_copy(layer, j, -step).wait_send()

            xz_copy(layer).wait_send()
            for j in range(2):
                y_copy(layer, j).wait_send()
                xy_copy(layer, j).wait_send()
            for q in range(4):
                core_copy(layer, cy, q).wait_send()
                core_copy(layer, 1 - cy, q).wait_send()

        both(s, act)
        return carry

    lax.fori_loop(1, layers, sent, 0)
    for k in range(4):
        own_copy(k).wait_send()
        core_copy(cl, 1 - cy, k).wait_send()

    def plane_copy(i):
        return pltpu.make_async_remote_copy(
            src_ref=plane_ref.at[spot],
            dst_ref=plane_ref.at[spot],
            send_sem=plane_send.at[i],
            recv_sem=plane_recv.at[spot],
            device_id=plane_peer(i),
            device_id_type=MESH,
        )

    def line_copy(i):
        return pltpu.make_async_remote_copy(
            src_ref=line_ref.at[cl],
            dst_ref=line_ref.at[cl],
            send_sem=line_send.at[i],
            recv_sem=line_recv.at[cl],
            device_id=line_peer(i),
            device_id_type=MESH,
        )

    def landed(ref, sem):
        pltpu.make_async_copy(ref, ref, sem).wait()

    for i in range(1, 8):
        plane_copy(i).start()
    for i in range(1, 8):
        source = (spot + i) % 8
        landed(plane_ref.at[source], plane_recv.at[source])
    line_ref[cl] = jnp.sum(plane_ref[...], axis=0)
    for i in range(1, 8):
        plane_copy(i).wait_send()

    def to_line(i, carry):
        line_copy(i).start()
        return carry

    def from_line(i, carry):
        source = (cl + i) % layers
        landed(line_ref.at[source], line_recv.at[source])
        line_copy(i).wait_send()
        return carry

    lax.fori_loop(1, layers, to_line, 0)
    lax.fori_loop(1, layers, from_line, 0)
    loss_ref[0, 0] = jnp.sum(line_ref[...]) / (tokens * layers * 2 * columns)


def per_device(fsdp, x, gain, codes, scales, outer, down, up, target):
    tokens, width = x.shape
    columns = up.shape[1]
    rows = codes.shape[0]
    layers = fsdp // 2
    vmem = pl.BlockSpec(memory_space=pltpu.VMEM)
    anywhere = pl.BlockSpec(memory_space=pl.ANY)
    dma = pltpu.SemaphoreType.DMA
    kv, loss = pl.pallas_call(
        functools.partial(kernel, layers),
        out_shape=(
            jax.ShapeDtypeStruct((tokens, columns), jnp.bfloat16),
            jax.ShapeDtypeStruct((1, 1), jnp.float32),
        ),
        in_specs=[anywhere, vmem, vmem, vmem, vmem, anywhere, vmem, anywhere],
        out_specs=(vmem, pl.BlockSpec(memory_space=pltpu.SMEM)),
        scratch_shapes=[
            pltpu.VMEM((tokens, width), jnp.bfloat16),
            pltpu.VMEM((width, columns), jnp.bfloat16),
            pltpu.VMEM((tokens, columns), jnp.float32),
            pltpu.VMEM((tokens, columns), jnp.bfloat16),
            pltpu.VMEM(down.shape[::-1], jnp.bfloat16),
            pltpu.VMEM((512, 512), jnp.bfloat16),
            pltpu.VMEM(codes.shape, jnp.float32),
            pltpu.VMEM((width // 128, 128), jnp.float32),
            pltpu.VMEM((8, 8, 128), jnp.float32),
            pltpu.VMEM((layers, 8, 128), jnp.float32),
            dma((6,)),
            dma((2 * layers * 3,)),
            dma((layers * 3,)),
            dma((layers * 2,)),
            dma((4,)),
            dma((layers * 8,)),
            dma((layers * 8,)),
            dma((layers * 8,)),
            dma((8,)),
            dma((8,)),
            dma((layers,)),
            dma((layers,)),
        ],
        compiler_params=pltpu.CompilerParams(
            collective_id=0, has_side_effects=True, vmem_limit_bytes=60 * 1024 * 1024
        ),
    )(x, gain.reshape(-1, 128), codes, scales, outer.reshape(1, -1), down.T, up, target)
    return kv, loss.reshape(())


def solution(mesh):
    placed = (
        P(("grp", "fsdp"), None),
        P(),
        P("fsdp", None),
        P("fsdp", None),
        P("fsdp"),
        P(),
        P(),
        P(("grp", "fsdp"), None),
    )
    return jax.shard_map(
        functools.partial(per_device, mesh.shape["fsdp"]),
        mesh=mesh,
        in_specs=placed,
        out_specs=(P(("grp", "fsdp"), None), P()),
        check_vma=False,
    )
```

```python
import functools

import jax
import jax.numpy as jnp
from jax import lax
from jax.experimental import pallas as pl
from jax.experimental.pallas import tpu as pltpu
from jax.sharding import PartitionSpec as P

adapter_scale = 0.25
epsilon = 1e-06
nf4_levels = (
    -1.0,
    -0.6961928009986877,
    -0.5250730514526367,
    -0.39491748809814453,
    -0.28444138169288635,
    -0.18477343022823334,
    -0.09105003625154495,
    0.0,
    0.07958029955625534,
    0.16093020141124725,
    0.24611230194568634,
    0.33791524171066284,
    0.44070982933044434,
    0.5626170039176941,
    0.7229568362236023,
    1.0,
)
MESH = pl.DeviceIdType.MESH


def nibble_levels(words, plane):
    values = [jnp.float32(level) for level in nf4_levels]
    for bit in range(4):
        is_set = jnp.bitwise_and(words, 1 << (4 * plane + bit)) != 0
        values = [
            jnp.where(is_set, values[2 * i + 1], values[2 * i])
            for i in range(len(values) // 2)
        ]
    return values[0]


def kernel(
    layers,
    x_hbm,
    gain_ref,
    codes_ref,
    scales_ref,
    outer_ref,
    down_hbm,
    up_ref,
    target_hbm,
    out_ref,
    loss_ref,
    x_ref,
    weight_ref,
    acc_ref,
    target_ref,
    down_ref,
    spread_ref,
    scale_ref,
    wide_gain_ref,
    plane_ref,
    line_ref,
    local_sem,
    z_send,
    x_send,
    y_send,
    own_send,
    core_send,
    link_recv,
    core_recv,
    plane_send,
    plane_recv,
    line_send,
    line_recv,
):
    g = lax.axis_index("grp")
    f = lax.axis_index("fsdp")
    cx, cc = g // 2, g % 2
    cl, cy = f // 2, f % 2
    tokens, width = x_ref.shape
    columns = acc_ref.shape[1]
    rows = codes_ref.shape[0]
    half = rows // 2
    piece = half // 4

    sibling = (cx * 2 + 1 - cc, f)
    x_peer = ((1 - cx) * 2 + cc, f)
    y_peer = (g, cl * 2 + 1 - cy)

    def z_peer(step):
        return (g, (cl + step) * 2 + cy)

    part = tokens // 4
    x_copies = [
        pltpu.make_async_copy(
            x_hbm.at[pl.ds(p * part, part)], x_ref.at[pl.ds(p * part, part)], local_sem.at[p]
        )
        for p in range(4)
    ]
    target_copy = pltpu.make_async_copy(target_hbm, target_ref, local_sem.at[4])
    down_copy = pltpu.make_async_copy(down_hbm, down_ref, local_sem.at[5])
    for copy in x_copies:
        copy.start()
    down_copy.start()
    target_copy.start()

    barrier = pltpu.get_barrier_semaphore()
    spot = (cx * 2 + cc) * 2 + cy

    def plane_peer(i):
        to = (spot + i) % 8
        return (to // 2, cl * 2 + to % 2)

    def line_peer(i):
        return (g, (cl + i) % layers * 2 + cy)

    for i in range(1, 8):
        pl.semaphore_signal(barrier, inc=1, device_id=plane_peer(i), device_id_type=MESH)

    def greet(i, carry):
        pl.semaphore_signal(barrier, inc=1, device_id=line_peer(i), device_id_type=MESH)
        return carry

    lax.fori_loop(1, layers, greet, 0)

    def mirror(px, j):
        return j + px * (3 - 2 * j)

    def chunk(layer, y, c, q):
        start = ((layer * 2 + y) * 2 + c) * half + q * piece
        return weight_ref.at[pl.ds(pl.multiple_of(start, piece), piece)]

    def slot(layer, y, q):
        return (layer * 2 + y) * 4 + q

    def link_copy(layer, y, q, send_sem, peer):
        ref = chunk(layer, y, cc, q)
        return pltpu.make_async_remote_copy(
            src_ref=ref,
            dst_ref=ref,
            send_sem=send_sem,
            recv_sem=link_recv.at[slot(layer, y, q)],
            device_id=peer,
            device_id_type=MESH,
        )

    def z_copy(layer, j, step):
        sem = z_send.at[(1 + step) // 2 * (layers * 3) + layer * 3 + j]
        return link_copy(layer, cy, mirror(cx, j), sem, z_peer(step))

    def xz_copy(layer):
        return link_copy(layer, cy, mirror(cx, 0), x_send.at[layer * 3], x_peer)

    def xy_copy(layer, j):
        return link_copy(layer, 1 - cy, mirror(cx, j), x_send.at[layer * 3 + 1 + j], x_peer)

    def y_copy(layer, j):
        return link_copy(layer, cy, mirror(cx, j), y_send.at[layer * 2 + j], y_peer)

    def own_copy(k):
        return link_copy(cl, cy, mirror(cx, k), own_send.at[k], y_peer)

    def core_copy(layer, y, q):
        ref = chunk(layer, y, cc, q)
        place = slot(layer, y, q)
        return pltpu.make_async_remote_copy(
            src_ref=ref,
            dst_ref=ref,
            send_sem=core_send.at[place],
            recv_sem=core_recv.at[place],
            device_id=sibling,
            device_id_type=MESH,
        )

    def arrived(layer, y, q):
        ref = chunk(layer, y, cc, q)
        pltpu.make_async_copy(ref, ref, link_recv.at[slot(layer, y, q)]).wait()

    def core_arrived(layer, y, q):
        ref = chunk(layer, y, 1 - cc, q)
        pltpu.make_async_copy(ref, ref, core_recv.at[slot(layer, y, q)]).wait()

    wide_gain_ref[...] = gain_ref[...].astype(jnp.float32)

    words = codes_ref.shape[1]
    lanes = scales_ref.shape[1]
    per_row = scales_ref.shape[0] * lanes // rows
    line = rows // scales_ref.shape[0]
    row = lax.broadcasted_iota(jnp.int32, (rows, lanes), 0)
    lane = lax.broadcasted_iota(jnp.int32, (rows, lanes), 1)
    mine = lane // per_row == row % line
    place = lax.broadcasted_iota(jnp.int32, (lanes, words), 0)
    word = lax.broadcasted_iota(jnp.int32, (lanes, words), 1)
    run = words // (4 * per_row)
    code = jnp.zeros((rows, words), jnp.float32)
    scale_words = jnp.concatenate(
        [
            jnp.broadcast_to(scales_ref[pl.ds(i, 1), :], (line, lanes))
            for i in range(scales_ref.shape[0])
        ],
        axis=0,
    )
    for byte in range(4):
        value = jnp.bitwise_and(jnp.right_shift(scale_words, 8 * byte), 255)
        value = jnp.where(mine, value.astype(jnp.float32), 0.0).astype(jnp.bfloat16)
        pick = (place % per_row == word // (4 * run)) & ((word // run) % 4 == byte)
        code += jnp.dot(
            value,
            jnp.where(pick, 1.0, 0.0).astype(jnp.bfloat16),
            preferred_element_type=jnp.float32,
        )
    outer_count = outer_ref.shape[1]
    outer_rows = rows // outer_count
    outer_row = lax.broadcasted_iota(jnp.int32, (rows, outer_count), 0)
    outer_lane = lax.broadcasted_iota(jnp.int32, (rows, outer_count), 1)
    second = jnp.sum(
        jnp.where(
            outer_row // outer_rows == outer_lane, outer_ref[...].astype(jnp.float32), 0.0
        ),
        axis=1,
        keepdims=True,
    )
    second = jnp.exp2(second / 128.0 - 6.0)
    scale_ref[...] = (code + 0.5) / 256.0 * second

    deep = lax.broadcasted_iota(jnp.int32, spread_ref.shape, 0)
    wide = lax.broadcasted_iota(jnp.int32, spread_ref.shape, 1)
    spread_ref[...] = jnp.where(
        (deep % 128) * 4 + deep // 128 == wide, 1.0, 0.0
    ).astype(jnp.bfloat16)

    def decode(start):
        start = pl.multiple_of(start, piece)
        for h in range(words // 128):
            span = pl.ds(h * 128, 128)
            code_words = codes_ref[pl.ds(start, piece), span]
            scale = scale_ref[pl.ds(start, piece), span]
            planes = [
                (nibble_levels(code_words, plane) * scale).astype(jnp.bfloat16)
                for plane in range(4)
            ]
            ordered = jnp.dot(
                jnp.concatenate(planes, axis=1),
                spread_ref[...],
                preferred_element_type=jnp.float32,
            )
            weight_ref[
                pl.ds(pl.multiple_of(f * rows + start, piece), piece), pl.ds(h * 512, 512)
            ] = ordered.astype(jnp.bfloat16)

    decode(cc * half + mirror(cx, 0) * piece)
    pl.semaphore_wait(barrier, 7 + layers - 1)

    def first_sends(j):
        @pl.when(cl > 0)
        def _():
            z_copy(cl, j, -1).start()

        @pl.when(cl < layers - 1)
        def _():
            z_copy(cl, j, 1).start()

        pl.when(j == 0)(lambda: own_copy(0).start())

    def rest(j, carry):
        decode(cc * half + mirror(cx, j) * piece)
        first_sends(j - 1)
        return carry

    lax.fori_loop(1, 4, rest, 0)
    for k in range(layers, 4):
        own_copy(k).start()

    def other(j, carry):
        decode((1 - cc) * half + j * piece)
        return carry

    lax.fori_loop(0, 4, other, 0)

    block = min(16, part)
    tile = min(1024, width)

    def normalize(p):
        x_copies[p].wait()

        def some(i, carry):
            at = pl.ds(pl.multiple_of(p * part + i * block, block), block)
            total = jnp.zeros((block, 128), jnp.float32)
            for t in range(width // tile):
                v = x_ref[at, pl.ds(t * tile, tile)].astype(jnp.float32)
                v = v * v
                for k in range(tile // 128):
                    total += v[:, k * 128 : (k + 1) * 128]
            inverse = lax.rsqrt(jnp.sum(total, axis=1, keepdims=True) / width + epsilon)
            for t in range(width // 128):
                span = pl.ds(t * 128, 128)
                v = x_ref[at, span].astype(jnp.float32)
                x_ref[at, span] = (v * inverse * wide_gain_ref[pl.ds(t, 1), :]).astype(jnp.bfloat16)
            return carry

        lax.fori_loop(0, part // block, some, 0)

    def adapter():
        down_copy.wait()
        low = lax.dot_general(
            x_ref[...],
            down_ref[...],
            (((1,), (1,)), ((), ())),
            preferred_element_type=jnp.float32,
        )
        acc_ref[...] = adapter_scale * jnp.dot(
            low.astype(jnp.bfloat16), up_ref[...], preferred_element_type=jnp.float32
        )

    across = min(256, columns)

    def multiply(layer, y):
        at = pl.ds(pl.multiple_of((layer * 2 + y) * rows, rows), rows)

        def some(n, carry):
            cols = pl.ds(pl.multiple_of(n * across, across), across)
            acc_ref[:, cols] += jnp.dot(
                x_ref[:, at], weight_ref[at, cols], preferred_element_type=jnp.float32
            )
            return carry

        lax.fori_loop(0, columns // across, some, 0)

    def multiply_arrived(layer, y):
        for q in range(4):
            core_arrived(layer, y, q)
        multiply(layer, y)

    def both(s, act):
        for step in (-1, 1):
            layer = cl + step * s
            pl.when((layer >= 0) & (layer < layers))(functools.partial(act, layer, step))

    def z_event(s, j):
        def act(layer, step):
            arrived(layer, cy, mirror(cx, j))
            onward = cl - step

            @pl.when((onward >= 0) & (onward < layers))
            def _():
                z_copy(layer, j, -step).start()

            if j == 0:
                xz_copy(layer).start()
            if j < 2:
                y_copy(layer, j).start()
            core_copy(layer, cy, mirror(cx, j)).start()

        both(s, act)

    def y_event(s, j):
        def act(layer, step):
            q = mirror(cx, j)
            arrived(layer, 1 - cy, q)
            xy_copy(layer, j).start()
            core_copy(layer, 1 - cy, q).start()

        both(s, act)

    def xz_event(s):
        def act(layer, step):
            q = mirror(1 - cx, 0)
            arrived(layer, cy, q)
            core_copy(layer, cy, q).start()

        both(s, act)

    def xy_event(s, j):
        def act(layer, step):
            q = mirror(1 - cx, j)
            arrived(layer, 1 - cy, q)
            core_copy(layer, 1 - cy, q).start()

        both(s, act)

    def own_event(k):
        q = mirror(cx, k)
        arrived(cl, 1 - cy, q)
        core_copy(cl, 1 - cy, q).start()

    def late(s):
        pl.when(s <= 4)(lambda: own_event(s - 1))
        xy_event(s - 1, 0)
        xy_event(s - 1, 1)

    def one_step(s, carry):
        z_event(s, 0)

        @pl.when(s > 1)
        def _():
            both(s - 1, lambda layer, step: multiply_arrived(layer, cy))

        @pl.when(s == 1)
        def _():
            normalize(0)
            normalize(1)

        z_event(s, 1)
        y_event(s, 0)
        pl.when(s > 1)(lambda: late(s))
        pl.when(s == 1)(lambda: own_event(0))

        @pl.when(s == 1)
        def _():
            normalize(2)
            normalize(3)

        z_event(s, 2)
        pl.when(s < 4)(lambda: own_copy(s).start())
        y_event(s, 1)
        xz_event(s)

        @pl.when(s > 1)
        def _():
            both(s - 1, lambda layer, step: multiply_arrived(layer, 1 - cy))

        @pl.when(s == 1)
        def _():
            adapter()
            multiply(cl, cy)

        return carry

    lax.fori_loop(1, layers, one_step, 0)
    xy_event(layers - 1, 0)
    both(layers - 1, lambda layer, step: multiply_arrived(layer, cy))
    for k in range(min(layers - 1, 4), 4):
        own_event(k)
    xy_event(layers - 1, 1)
    multiply_arrived(cl, 1 - cy)
    both(layers - 1, lambda layer, step: multiply_arrived(layer, 1 - cy))

    target_copy.wait()
    plane_ref[spot] = jnp.zeros((8, 128), jnp.float32)

    def finish(i, carry):
        at = pl.ds(pl.multiple_of(i * block, block), block)
        exact = acc_ref[at, :]
        out_ref[at, :] = exact.astype(jnp.bfloat16)
        error = exact - target_ref[at, :].astype(jnp.float32)
        error = error * error
        total = jnp.zeros((block, 128), jnp.float32)
        for k in range(columns // 128):
            total += error[:, k * 128 : (k + 1) * 128]
        for k in range(block // 8):
            plane_ref[spot] += total[k * 8 : (k + 1) * 8]
        return carry

    lax.fori_loop(0, tokens // block, finish, 0)

    for j in range(3):
        for step in (-1, 1):

            @pl.when((cl + step >= 0) & (cl + step < layers))
            def _():
                z_copy(cl, j, step).wait_send()

    def sent(s, carry):
        def act(layer, step):
            onward = cl - step

            @pl.when((onward >= 0) & (onward < layers))
            def _():
                for j in range(3):
                    z_copy(layer, j, -step).wait_send()

            xz_copy(layer).wait_send()
            for j in range(2):
                y_copy(layer, j).wait_send()
                xy_copy(layer, j).wait_send()
            for q in range(4):
                core_copy(layer, cy, q).wait_send()
                core_copy(layer, 1 - cy, q).wait_send()

        both(s, act)
        return carry

    lax.fori_loop(1, layers, sent, 0)
    for k in range(4):
        own_copy(k).wait_send()
        core_copy(cl, 1 - cy, k).wait_send()

    def plane_copy(i):
        return pltpu.make_async_remote_copy(
            src_ref=plane_ref.at[spot],
            dst_ref=plane_ref.at[spot],
            send_sem=plane_send.at[i],
            recv_sem=plane_recv.at[spot],
            device_id=plane_peer(i),
            device_id_type=MESH,
        )

    def line_copy(i):
        return pltpu.make_async_remote_copy(
            src_ref=line_ref.at[cl],
            dst_ref=line_ref.at[cl],
            send_sem=line_send.at[i],
            recv_sem=line_recv.at[cl],
            device_id=line_peer(i),
            device_id_type=MESH,
        )

    def landed(ref, sem):
        pltpu.make_async_copy(ref, ref, sem).wait()

    for i in range(1, 8):
        plane_copy(i).start()
    for i in range(1, 8):
        source = (spot + i) % 8
        landed(plane_ref.at[source], plane_recv.at[source])
    line_ref[cl] = jnp.sum(plane_ref[...], axis=0)
    for i in range(1, 8):
        plane_copy(i).wait_send()

    def to_line(i, carry):
        line_copy(i).start()
        return carry

    def from_line(i, carry):
        source = (cl + i) % layers
        landed(line_ref.at[source], line_recv.at[source])
        line_copy(i).wait_send()
        return carry

    lax.fori_loop(1, layers, to_line, 0)
    lax.fori_loop(1, layers, from_line, 0)
    loss_ref[0, 0] = jnp.sum(line_ref[...]) / (tokens * layers * 2 * columns)


def per_device(fsdp, x, gain, codes, scales, outer, down, up, target):
    tokens, width = x.shape
    columns = up.shape[1]
    rows = codes.shape[0]
    layers = fsdp // 2
    vmem = pl.BlockSpec(memory_space=pltpu.VMEM)
    anywhere = pl.BlockSpec(memory_space=pl.ANY)
    dma = pltpu.SemaphoreType.DMA
    kv, loss = pl.pallas_call(
        functools.partial(kernel, layers),
        out_shape=(
            jax.ShapeDtypeStruct((tokens, columns), jnp.bfloat16),
            jax.ShapeDtypeStruct((1, 1), jnp.float32),
        ),
        in_specs=[anywhere, vmem, vmem, vmem, vmem, anywhere, vmem, anywhere],
        out_specs=(vmem, pl.BlockSpec(memory_space=pltpu.SMEM)),
        scratch_shapes=[
            pltpu.VMEM((tokens, width), jnp.bfloat16),
            pltpu.VMEM((width, columns), jnp.bfloat16),
            pltpu.VMEM((tokens, columns), jnp.float32),
            pltpu.VMEM((tokens, columns), jnp.bfloat16),
            pltpu.VMEM(down.shape[::-1], jnp.bfloat16),
            pltpu.VMEM((512, 512), jnp.bfloat16),
            pltpu.VMEM(codes.shape, jnp.float32),
            pltpu.VMEM((width // 128, 128), jnp.float32),
            pltpu.VMEM((8, 8, 128), jnp.float32),
            pltpu.VMEM((layers, 8, 128), jnp.float32),
            dma((6,)),
            dma((2 * layers * 3,)),
            dma((layers * 3,)),
            dma((layers * 2,)),
            dma((4,)),
            dma((layers * 8,)),
            dma((layers * 8,)),
            dma((layers * 8,)),
            dma((8,)),
            dma((8,)),
            dma((layers,)),
            dma((layers,)),
        ],
        compiler_params=pltpu.CompilerParams(
            collective_id=0, has_side_effects=True, vmem_limit_bytes=60 * 1024 * 1024
        ),
    )(x, gain.reshape(-1, 128), codes, scales, outer.reshape(1, -1), down.T, up, target)
    return kv, loss.reshape(())


def solution(mesh):
    placed = (
        P(("grp", "fsdp"), None),
        P(),
        P("fsdp", None),
        P("fsdp", None),
        P("fsdp"),
        P(),
        P(),
        P(("grp", "fsdp"), None),
    )
    return jax.shard_map(
        functools.partial(per_device, mesh.shape["fsdp"]),
        mesh=mesh,
        in_specs=placed,
        out_specs=(P(("grp", "fsdp"), None), P()),
        check_vma=False,
    )
```
